32 devices in a mesh: tg: 2 (over core), pw: 16 (over z, y, x).
Axes of the slice: x: 2, y: 2, z: 4, core: 2. Of those that a mesh axis runs over, the one named last changes fastest.
Arguments:
- coeffs: float32 [2, 8192, 256], P(None, ('tg', 'pw')), may hold values from -6 to 6
- g_place: int32 [8192], P(('tg', 'pw')), may hold values from 0 to 2047, as said below
- stick_column: int32 [512], P(('tg', 'pw')), may hold values from 0 to 16383, as said below
- potential: float32 [128, 128, 128], P(None, None, ('tg', 'pw')), may hold values from -1 to 3
Outputs:
- hpsi: float32 [2, 8192, 256], P(None, ('tg', 'pw'))
The draws below stay inside these ranges and needn't reach their ends.
Inputs may be any that keep to these rules, and one draw needn't show every extreme that they name: g_place[g] = s * 128 + z: s is a stick slot of the owner g // 256, z a frequency within 32 of zero taken modulo 128; no two plane waves of one owner share s and z; each owner uses its slots 0 up to some count between 4 and 16, every one of them, and some owner uses all 16. `stick_column`: all stick slots name different columns x * 128 + y; with x and y read as signed frequencies (taken modulo 128), x * x + y * y <= 32 ** 2.
All inputs are finite; a program needn't handle non-finite values.
Results may differ from the reference program's by a relative error of at most 0.009.
Values may be sent and summed in bfloat16 or wider, within the bound.
A program may use at most 256 MiB of HBM per device.

```python
import jax
import jax.numpy as jnp
from jax import lax

NR = 128
ZSPAN = 64
SLOT = 16
G_DEV = 256
BANDS = 256
G_TOTAL = 8192
STICKS = 512


def live_slots(key):
    owners = STICKS // SLOT
    random_part = SLOT // 4 + jax.random.randint(jax.random.fold_in(key, 11), (owners,), 0, SLOT - SLOT // 4 + 1)
    busiest = jax.random.randint(jax.random.fold_in(key, 12), (), 0, owners)
    return jnp.where(jnp.arange(owners) == busiest, SLOT, random_part)


def draw_g_place(key, part):
    owners = STICKS // SLOT
    cell_count = SLOT * ZSPAN
    live_count = live_slots(key)
    position = jnp.arange(cell_count, dtype=jnp.int32)
    slot_of = position // ZSPAN
    random_part = jax.random.randint(jax.random.fold_in(key, 13), (owners, cell_count), 0, 2 ** 20)
    scores = random_part * cell_count + position[None, :]
    scores = jnp.where(position[None, :] % ZSPAN == 0, 2 ** 30 + position[None, :], scores)
    scores = jnp.where(slot_of[None, :] < live_count[:, None], scores, -1 - position[None, :])
    chosen = lax.top_k(scores, G_DEV)[1]
    frequency = chosen % ZSPAN - ZSPAN // 2
    placed = chosen // ZSPAN * NR + jnp.mod(frequency, NR)
    return placed.reshape(G_TOTAL).astype(jnp.int32)


def draw_stick_column(key, part):
    radius = ZSPAN // 2
    side_length = ZSPAN + 1
    cell_count = side_length * side_length
    position = jnp.arange(cell_count, dtype=jnp.int32)
    x_signed = position // side_length - radius
    y_signed = position % side_length - radius
    inside = x_signed * x_signed + y_signed * y_signed <= radius * radius
    random_part = jax.random.randint(jax.random.fold_in(key, 21), (cell_count,), 0, 2 ** 16)
    scores = jnp.where(inside, random_part * cell_count + position, -1 - position)
    chosen = lax.top_k(scores, STICKS)[1]
    x_index = jnp.mod(x_signed[chosen], NR)
    y_index = jnp.mod(y_signed[chosen], NR)
    return (x_index * NR + y_index).astype(jnp.int32)


def shard_levels(stream_key, extent, shards, low, high):
    def one(axis_at, parts):
        heights = jax.random.uniform(jax.random.fold_in(jax.random.fold_in(stream_key, 6), axis_at), (parts,), jnp.float32, low / len(shards), high / len(shards))
        return jnp.repeat(jnp.exp(heights), extent[axis_at] // parts).reshape((-1,) + (1,) * (len(extent) - axis_at - 1))

    level = one(*shards[0])
    for cut in shards[1:]:
        level = level * one(*cut)
    return level


def bell_draw(stream_key, shape, deviation, most, shards=(), kind=jnp.bfloat16):
    result = deviation * jax.random.normal(stream_key, shape, jnp.float32)
    if shards:
        result = result * shard_levels(stream_key, shape, shards, -0.22, 0.18)
    return jnp.clip(result, -most, most).astype(kind)


def setup_inputs(seed: int = 0) -> dict:
    seeds = jax.random.split(jax.random.key(seed), 5)
    return {
        "coeffs": bell_draw(seeds[0], (2, G_TOTAL, BANDS), 1.0, 6.0, ((1, 32),), jnp.float32),
        "g_place": draw_g_place(jax.random.fold_in(seeds[4], 71), 0),
        "stick_column": draw_stick_column(jax.random.fold_in(seeds[4], 71), 0),
        "potential": jnp.clip(-1.0 + 4.0 * jax.random.uniform(seeds[3], (NR, NR, NR), jnp.float32) ** shard_levels(seeds[3], (NR, NR, NR), ((2, 32),), -0.2, 0.2), -1.0, 3.0),
    }


def phase_table(left_index, right_index, sign_value, modulus):
    product = (left_index[:, None] * right_index[None, :]) % modulus
    angles = (2.0 * jnp.pi / modulus) * product.astype(jnp.float32)
    cosine = jnp.cos(angles)
    sine_part = sign_value * jnp.sin(angles)
    upper_row = jnp.stack([cosine, sine_part])
    lower_row = jnp.stack([-sine_part, cosine])
    return jnp.stack([upper_row, lower_row])


def plane_pass(lattice, volume, forward, inverse):
    ahead = forward.astype(jnp.float32)
    behind = inverse.astype(jnp.float32)
    partial_value = jnp.einsum('cxypb,cdyk->dxkpb', lattice.astype(jnp.float32), ahead).astype(jnp.bfloat16)
    psi_field = jnp.einsum('cxypb,cdxk->dkypb', partial_value.astype(jnp.float32), ahead)
    weighted = (psi_field * volume[None, :, :, :, None]).astype(jnp.bfloat16)
    reverse_half = jnp.einsum('cxypb,cdyk->dxkpb', weighted.astype(jnp.float32), behind).astype(jnp.bfloat16)
    return jnp.einsum('cxypb,cdxk->dkypb', reverse_half.astype(jnp.float32), behind)


def reference(coeffs, g_place, stick_column, potential):
    frequency = jnp.arange(NR, dtype=jnp.int32)
    forward = phase_table(frequency, frequency, 1.0, NR).astype(jnp.bfloat16)
    inverse = phase_table(frequency, frequency, -1.0, NR).astype(jnp.bfloat16)
    ahead_table = phase_table(frequency, frequency, 1.0, NR)
    return_table = phase_table(frequency, frequency, -1.0, NR)
    holder = (jnp.arange(G_TOTAL, dtype=jnp.int32) // G_DEV).astype(jnp.int32)
    flat_index = (holder * (SLOT * NR) + g_place).astype(jnp.int32)
    factor = 1.0 / NR ** 3

    def one_band(band_values):
        placed = jnp.zeros((2, STICKS * NR), jnp.float32).at[:, flat_index].add(band_values)
        placed = placed.reshape(2, STICKS, NR)
        sticks = jnp.einsum('csz,cdzk->dsk', placed, ahead_table, precision=lax.Precision.HIGHEST).astype(jnp.bfloat16)
        lattice = jnp.zeros((2, NR * NR, NR), jnp.bfloat16).at[:, stick_column].set(sticks)
        real_image = plane_pass(lattice.reshape(2, NR, NR, NR, 1), potential, forward, inverse)
        picked = real_image.reshape(2, NR * NR, NR)[:, stick_column].astype(jnp.bfloat16)
        spectra = jnp.einsum('csz,cdzk->dsk', picked.astype(jnp.float32), return_table, precision=lax.Precision.HIGHEST)
        return spectra.reshape(2, STICKS * NR)[:, flat_index] * factor

    stacked = lax.map(one_band, jnp.transpose(coeffs, (2, 0, 1)))
    return jnp.transpose(stacked, (1, 2, 0))
```

```python
import jax
import jax.numpy as jnp
import numpy as np
from jax import lax
from jax.experimental import pallas as pl
from jax.experimental.pallas import tpu as pltpu
from jax.sharding import PartitionSpec as P

NR = 128
ZSPAN = 64
HALF = ZSPAN // 2
SIDE = ZSPAN + 1
PAD = 72
PITCH = 148
WIN = 80
BLOCK = 256
GROUP = 8
STEP = 13
OWNERS = 4
AXES = ("tg", "pw")
F32 = jnp.float32
BF16 = jnp.bfloat16


def unit_tables(left, right):
    angles = 2.0 * np.pi / NR * ((left[:, None] * right[None, :]) % NR)
    return np.cos(angles), np.sin(angles)


def plane_tables():
    full = np.arange(NR)
    cosine, sine = unit_tables(full, np.arange(SIDE) - HALF)
    pad = ((0, 0), (0, PAD - SIDE))
    cosine, sine = np.pad(cosine, pad), np.pad(sine, pad)
    ahead = np.block([[cosine, -sine], [sine, cosine]])
    cos_box, sin_box = unit_tables(full - HALF, full)
    made = (
        ahead,
        ahead.T,
        np.concatenate([cos_box, sin_box], 1),
        np.concatenate([-sin_box, cos_box], 1),
    )
    return tuple(jnp.asarray(table, BF16) for table in made)


def depth_tables(copies):
    planes = NR // copies
    made = []
    for copy in range(copies):
        cosine, sine = unit_tables(np.arange(NR), np.arange(planes) + copy * planes)
        turn = np.zeros((copies, 2, NR, 2, copies, planes))
        for band in range(copies):
            turn[band, 0, :, 0, band] = cosine
            turn[band, 0, :, 1, band] = sine
            turn[band, 1, :, 0, band] = -sine
            turn[band, 1, :, 1, band] = cosine
        made.append(turn.reshape(copies * 2 * NR, 2 * NR))
    return np.stack(made)


def dot(left, right):
    return jnp.dot(left, right, preferred_element_type=F32)


def dot_nt(left, right):
    return lax.dot_general(left, right, (((1,), (1,)), ((), ())), preferred_element_type=F32)


def hot(flags):
    return flags.astype(F32).astype(BF16)


def masks(mine_ref, owner, parts, slots):
    waves = mine_ref.shape[2]
    marks = mine_ref[owner, parts:parts + 8, :].astype(F32)
    depth = lax.broadcasted_iota(jnp.int32, (NR, waves), 0).astype(F32) == marks[1:2]
    slot = lax.broadcasted_iota(jnp.int32, (slots, waves), 0).astype(F32) == marks[0:1]
    return hot(depth), slot


def permute(source, target, index_ref):
    sticks = source.shape[1]

    def one(step, carry):
        rows = pl.ds(pl.multiple_of(step * BLOCK, BLOCK), BLOCK)
        wanted = lax.broadcasted_iota(jnp.int32, (BLOCK, sticks), 0) + step * BLOCK
        choice = hot(wanted == index_ref[...])
        for part in range(2):
            for chunk in range(source.shape[2] // BLOCK):
                lanes = pl.ds(chunk * BLOCK, BLOCK)
                target[part, rows, lanes] = dot(choice, source[part, :, lanes].astype(BF16)).astype(BF16)
        return carry

    lax.fori_loop(0, sticks // BLOCK, one, 0)


def rise_kernel(mine_ref, rank_ref, depth_ref, packed_ref, loose):
    owners = mine_ref.shape[0]
    parts = mine_ref.shape[1] - 8
    slots = rank_ref.shape[1] // owners
    bands = parts // 2
    twin = depth_ref.shape[0] // (2 * NR)

    def spread(step, carry):
        placed = []
        for inner in range(OWNERS):
            owner = step * OWNERS + inner
            depth, slot = masks(mine_ref, owner, parts, slots)
            values = mine_ref[owner, :parts, :].astype(F32)
            rows = [jnp.where(slot, values[part:part + 1], 0.0) for part in range(parts)]
            placed.append(dot_nt(jnp.concatenate(rows, 0).astype(BF16), depth).astype(BF16))
        turned = []
        for inner in range(OWNERS):
            rows = []
            for pair in range(bands // twin):
                cells = []
                for band in range(twin):
                    for part in range(2):
                        at = (part * bands + pair * twin + band) * slots
                        cells.append(placed[inner][at:at + slots])
                rows.append(jnp.concatenate(cells, 1))
            turned.append(dot(jnp.concatenate(rows, 0), depth_ref[...]).astype(BF16))
        for inner in range(OWNERS):
            where = pl.ds(pl.multiple_of((step * OWNERS + inner) * slots, slots), slots)
            for part in range(2):
                for pair in range(bands // twin):
                    loose[part, where, pl.ds(pair * NR, NR)] = turned[inner][
                        pair * slots:(pair + 1) * slots, part * NR:(part + 1) * NR
                    ]
        return carry

    lax.fori_loop(0, owners // OWNERS, spread, 0)
    permute(loose, packed_ref, rank_ref)


def plane_kernel(
    near_ref, close_ref, mine_ref, order_ref, xs_ref, ys_ref, packed, volume_ref,
    ahead_ref, behind_ref, first_ref, second_ref, depth_ref,
    out_ref,
    loose, picked, mixer, work, level, rows_one, rows_two, held,
):
    owners = mine_ref.shape[0]
    parts = mine_ref.shape[1] - 8
    waves = mine_ref.shape[2]
    sticks = order_ref.shape[1]
    slots = sticks // owners
    bands = parts // 2
    twin = depth_ref.shape[1] // (2 * NR)

    def make_rows(step, carry):
        rows = pl.ds(pl.multiple_of(step * BLOCK, BLOCK), BLOCK)
        choice = hot(lax.broadcasted_iota(jnp.int32, (BLOCK, NR), 1) == xs_ref[rows, :])
        rows_one[rows, :] = dot(choice, first_ref[...]).astype(BF16)
        rows_two[rows, :] = dot(choice, second_ref[...]).astype(BF16)
        return carry

    lax.fori_loop(0, sticks // BLOCK, make_rows, 0)

    def make_mixer(step, carry):
        for inner in range(5):
            y = step * 5 + inner
            rows = pl.ds(pl.multiple_of(near_ref[y], 16), NR)
            mine = ys_ref[rows, :] == y
            mine = jnp.concatenate([mine, mine], 1)
            one = jnp.where(mine, rows_one[rows, :].astype(F32), 0.0)
            two = jnp.where(mine, rows_two[rows, :].astype(F32), 0.0)
            mixer[y] = jnp.concatenate([one.T, two.T], 1).astype(BF16)
        return carry

    lax.fori_loop(0, SIDE // 5, make_mixer, 0)

    def make_level(step, carry):
        for inner in range(8):
            rx = step * 8 + inner
            rows = [volume_ref[holder, rx].astype(F32) for holder in range(volume_ref.shape[0])]
            level[rx] = jnp.concatenate(rows * twin, 0).T
        return carry

    lax.fori_loop(0, NR // 8, make_level, 0)

    for half in range(2):
        for part in range(2):
            for row in range(SIDE, PAD):
                work[half, pl.ds(part * PAD + row, NR, stride=PITCH), :] = jnp.zeros((NR, NR), F32)

    def rows_of(step, inner):
        return pl.ds((step * GROUP + inner) * PITCH, 2 * PAD)

    def lift(step):
        data = []
        for inner in range(GROUP):
            rows = rows_of(step, inner)
            data.append(jnp.concatenate([work[0, rows, :], work[1, rows, :]], 1).astype(BF16))
        for inner in range(GROUP):
            psi = dot(ahead_ref[...], data[inner])
            here = level[step * GROUP + inner]
            here = jnp.concatenate([here, here], 1)
            here = jnp.concatenate([here, here], 0)
            held[inner] = (psi * here).astype(BF16)

    def fall():
        return [dot(behind_ref[...], held[inner]) for inner in range(GROUP)]

    def put(step, results):
        for inner in range(GROUP):
            rows = rows_of(step, inner)
            work[0, rows, :] = results[inner][:, :NR]
            work[1, rows, :] = results[inner][:, NR:]

    def tile(index, carry):
        lanes = pl.ds(pl.multiple_of(index * BLOCK, BLOCK), BLOCK)

        def stage_one(step, carry):
            results = []
            for inner in range(STEP):
                y = step * STEP + inner
                rows = pl.ds(pl.multiple_of(near_ref[y], 16), NR)
                data = jnp.concatenate([packed[0, rows, lanes], packed[1, rows, lanes]], 0)
                results.append(dot(mixer[y], data))
            for inner in range(STEP):
                y = step * STEP + inner
                for half in range(2):
                    for part in range(2):
                        work[half, pl.ds(part * PAD + y, NR, stride=PITCH), :] = results[inner][
                            part * NR:(part + 1) * NR, half * NR:(half + 1) * NR
                        ]
            return carry

        lax.fori_loop(0, SIDE // STEP, stage_one, 0)

        def stage_two(step, carry):
            results = fall()
            lift(step)
            put(step - 1, results)
            return carry

        lift(0)
        lax.fori_loop(1, NR // GROUP, stage_two, 0)
        put(NR // GROUP - 1, fall())

        def stage_three(step, carry):
            results = []
            for inner in range(STEP):
                y = step * STEP + inner
                data = [
                    jnp.concatenate(
                        [work[half, pl.ds(part * PAD + y, NR, stride=PITCH), :] for half in range(2)], 1
                    )
                    for part in range(2)
                ]
                data = jnp.concatenate(data, 0).astype(BF16)
                rows = pl.ds(pl.multiple_of(close_ref[y], 16), WIN)
                weights = jnp.concatenate([rows_one[rows, :], rows_two[rows, :]], 0)
                results.append(dot(weights, data))
            for inner in range(STEP):
                y = step * STEP + inner
                rows = pl.ds(pl.multiple_of(close_ref[y], 16), WIN)
                mine = ys_ref[rows, :] == y
                mine = jnp.concatenate([mine, mine], 1)
                for part in range(2):
                    picked[part, rows, lanes] = jnp.where(
                        mine, results[inner][part * WIN:(part + 1) * WIN], picked[part, rows, lanes]
                    )
            return carry

        lax.fori_loop(0, SIDE // STEP, stage_three, 0)
        return carry

    lax.fori_loop(0, packed.shape[2] // BLOCK, tile, 0)

    permute(picked, loose, order_ref)

    def collect(step, carry):
        total = hot(
            lax.broadcasted_iota(jnp.int32, (parts, parts * slots), 1) // slots
            == lax.broadcasted_iota(jnp.int32, (parts, parts * slots), 0)
        )
        turned = []
        for inner in range(OWNERS):
            where = pl.ds(pl.multiple_of((step * OWNERS + inner) * slots, slots), slots)
            rows = []
            for pair in range(bands // twin):
                here = pl.ds(pair * NR, NR)
                rows.append(jnp.concatenate([loose[0, where, here], loose[1, where, here]], 1))
            turned.append(dot(jnp.concatenate(rows, 0), depth_ref[...]).astype(BF16))
        waved = []
        for inner in range(OWNERS):
            depth, slot = masks(mine_ref, step * OWNERS + inner, parts, slots)
            rows = []
            for part in range(2):
                for pair in range(bands // twin):
                    for band in range(twin):
                        at = (band * 2 + part) * NR
                        rows.append(turned[inner][pair * slots:(pair + 1) * slots, at:at + NR])
            found = dot(jnp.concatenate(rows, 0), depth)
            slot = jnp.concatenate([slot] * parts, 0)
            waved.append(jnp.where(slot, found, 0.0).astype(BF16))
        for inner in range(OWNERS):
            out_ref[step * OWNERS + inner] = dot(total, waved[inner]).astype(BF16)
        return carry

    lax.fori_loop(0, owners // OWNERS, collect, 0)


def body(coeffs, g_place, stick_column, potential):
    groups = lax.axis_size("tg")
    columns = lax.axis_size("pw")
    owners = groups * columns
    waves = g_place.shape[0]
    slots = stick_column.shape[0]
    bands = coeffs.shape[2] // columns
    sticks = owners * slots
    parts = 2 * bands

    local = potential.transpose(0, 2, 1).astype(BF16)[None]
    volume = lax.all_gather(local, "pw", axis=0, tiled=True)

    sent = coeffs.astype(BF16).transpose(2, 0, 1).reshape(columns, bands, 2, waves)
    sent = sent.transpose(0, 2, 1, 3).reshape(columns, parts, waves)
    marks = jnp.stack(
        [
            g_place // NR,
            g_place % NR,
            jnp.pad(stick_column // NR, (0, waves - slots)),
            jnp.pad(stick_column % NR, (0, waves - slots)),
        ]
    )
    marks = jnp.pad(marks, ((0, 4), (0, 0))).astype(BF16)
    marks = jnp.broadcast_to(marks[None], (columns, 8, waves))
    sent = jnp.concatenate([sent, marks], 1)
    sent = jnp.broadcast_to(sent[None], (groups,) + sent.shape).reshape(owners, parts + 8, waves)
    mine = lax.all_to_all(sent, AXES, split_axis=0, concat_axis=0, tiled=True)

    sites = mine[:, parts + 2:parts + 4, :slots].astype(F32).astype(jnp.int32)
    xs = jnp.bitwise_and(sites[:, 0].reshape(sticks) + HALF, NR - 1)
    ys = jnp.bitwise_and(sites[:, 1].reshape(sticks) + HALF, NR - 1)
    key = ys * NR + xs
    rank = jnp.sum((key[None, :] < key[:, None]).astype(jnp.int32), 1)
    spot = jnp.arange(sticks, dtype=jnp.int32)
    hit = rank[None, :] == spot[:, None]
    order = jnp.sum(jnp.where(hit, spot[None, :], 0), 1)
    sorted_key = jnp.sum(jnp.where(hit, key[None, :], 0), 1)
    wide = jnp.broadcast_to(sorted_key[:, None], (sticks, NR))
    starts = jnp.sum((ys[None, :] < jnp.arange(SIDE)[:, None]).astype(jnp.int32), 1) // 16 * 16
    near = jnp.minimum(starts, sticks - NR)
    close = jnp.minimum(starts, sticks - WIN)

    depth = depth_tables(groups)
    turn = lax.axis_index("tg")
    depth_ahead = jnp.asarray(depth, BF16)[turn]
    depth_behind = jnp.asarray(depth.transpose(0, 2, 1), BF16)[turn]

    smem = pl.BlockSpec(memory_space=pltpu.SMEM)
    vmem = pl.BlockSpec(memory_space=pltpu.VMEM)
    lanes = bands * (NR // groups)
    packed = pl.pallas_call(
        rise_kernel,
        out_shape=jax.ShapeDtypeStruct((2, sticks, lanes), BF16),
        in_specs=[vmem] * 3,
        out_specs=vmem,
        scratch_shapes=[pltpu.VMEM((2, sticks, lanes), BF16)],
        compiler_params=pltpu.CompilerParams(vmem_limit_bytes=48 * 2**20),
        cost_estimate=pl.CostEstimate(flops=2 * 10**10, bytes_accessed=4 * 2**20, transcendentals=0),
        name="rise",
    )(mine, rank[None, :], depth_ahead)

    made = pl.pallas_call(
        plane_kernel,
        out_shape=jax.ShapeDtypeStruct((owners, parts, waves), BF16),
        in_specs=[smem, smem] + [vmem] * 11,
        out_specs=vmem,
        scratch_shapes=[
            pltpu.VMEM((2, sticks, lanes), BF16),
            pltpu.VMEM((2, sticks, lanes), F32),
            pltpu.VMEM((SIDE, 2 * NR, 2 * NR), BF16),
            pltpu.VMEM((2, NR * PITCH, NR), F32),
            pltpu.VMEM((NR, NR, NR), F32),
            pltpu.VMEM((sticks, 2 * NR), BF16),
            pltpu.VMEM((sticks, 2 * NR), BF16),
            pltpu.VMEM((GROUP, 2 * NR, 2 * NR), BF16),
        ],
        compiler_params=pltpu.CompilerParams(vmem_limit_bytes=60 * 2**20),
        cost_estimate=pl.CostEstimate(flops=8 * 10**10, bytes_accessed=8 * 2**20, transcendentals=0),
        name="planes",
    )(
        near, close, mine, order[None, :],
        jnp.bitwise_and(wide, NR - 1), wide // NR, packed, volume, *plane_tables(), depth_behind,
    )

    back = lax.all_to_all(made, AXES, split_axis=0, concat_axis=0, tiled=True)
    back = jnp.sum(back.reshape(groups, columns, 2, bands, waves).astype(F32), 0)
    back = back.transpose(1, 3, 0, 2).reshape(2, waves, columns * bands)
    return back * (1.0 / NR**3)


def solution(mesh):
    placed = (P(None, AXES, None), P(AXES), P(AXES), P(None, None, AXES))
    return jax.shard_map(
        body, mesh=mesh, in_specs=placed, out_specs=P(None, AXES, None), check_vma=False
    )
```

```python
import jax
import jax.numpy as jnp
import numpy as np
from jax import lax
from jax.experimental import pallas as pl
from jax.experimental.pallas import tpu as pltpu
from jax.sharding import PartitionSpec as P


NR = 128
ZSPAN = 64
HALF = ZSPAN // 2
SIDE = ZSPAN + 1
PAD = 72
PITCH = 148
WIN = 80
BLOCK = 256
STEP = 13
OWNERS = 4
AXES = ("tg", "pw")
F32 = jnp.float32
BF16 = jnp.bfloat16


def unit_tables(left, right):
    angles = 2.0 * np.pi / NR * ((left[:, None] * right[None, :]) % NR)
    return np.cos(angles), np.sin(angles)


def plane_tables():
    full = np.arange(NR)
    cosine, sine = unit_tables(full, np.arange(SIDE) - HALF)
    pad = ((0, 0), (0, PAD - SIDE))
    cosine, sine = np.pad(cosine, pad), np.pad(sine, pad)
    ahead = np.block([[cosine, -sine], [sine, cosine]])
    cos_box, sin_box = unit_tables(full - HALF, full)
    made = (
        ahead,
        ahead.T,
        np.concatenate([cos_box, sin_box], 1),
        np.concatenate([-sin_box, cos_box], 1),
    )
    return tuple(jnp.asarray(table, BF16) for table in made)


def depth_tables(copies):
    planes = NR // copies
    made = []
    for copy in range(copies):
        cosine, sine = unit_tables(np.arange(NR), np.arange(planes) + copy * planes)
        turn = np.zeros((copies, 2, NR, 2, copies, planes))
        for band in range(copies):
            turn[band, 0, :, 0, band] = cosine
            turn[band, 0, :, 1, band] = sine
            turn[band, 1, :, 0, band] = -sine
            turn[band, 1, :, 1, band] = cosine
        made.append(turn.reshape(copies * 2 * NR, 2 * NR))
    return np.stack(made)


def dot(left, right):
    return jnp.dot(left, right, preferred_element_type=F32)


def dot_nt(left, right):
    return lax.dot_general(left, right, (((1,), (1,)), ((), ())), preferred_element_type=F32)


def hot(flags):
    return flags.astype(F32).astype(BF16)


def masks(mine_ref, owner, parts, slots):
    waves = mine_ref.shape[2]
    marks = mine_ref[owner, parts:parts + 8, :].astype(F32)
    depth = lax.broadcasted_iota(jnp.int32, (NR, waves), 0).astype(F32) == marks[1:2]
    slot = lax.broadcasted_iota(jnp.int32, (slots, waves), 0).astype(F32) == marks[0:1]
    return hot(depth), slot


def permute(source, target, index_ref):
    sticks = source.shape[1]

    def one(step, carry):
        rows = pl.ds(pl.multiple_of(step * BLOCK, BLOCK), BLOCK)
        wanted = lax.broadcasted_iota(jnp.int32, (BLOCK, sticks), 0) + step * BLOCK
        choice = hot(wanted == index_ref[...])
        for part in range(2):
            for chunk in range(source.shape[2] // BLOCK):
                lanes = pl.ds(chunk * BLOCK, BLOCK)
                target[part, rows, lanes] = dot(choice, source[part, :, lanes].astype(BF16)).astype(BF16)
        return carry

    lax.fori_loop(0, sticks // BLOCK, one, 0)


def rise_kernel(mine_ref, rank_ref, depth_ref, packed_ref, loose):
    owners = mine_ref.shape[0]
    parts = mine_ref.shape[1] - 8
    slots = rank_ref.shape[1] // owners
    bands = parts // 2
    twin = depth_ref.shape[0] // (2 * NR)

    def spread(step, carry):
        placed = []
        for inner in range(OWNERS):
            owner = step * OWNERS + inner
            depth, slot = masks(mine_ref, owner, parts, slots)
            values = mine_ref[owner, :parts, :].astype(F32)
            rows = [jnp.where(slot, values[part:part + 1], 0.0) for part in range(parts)]
            placed.append(dot_nt(jnp.concatenate(rows, 0).astype(BF16), depth).astype(BF16))
        turned = []
        for inner in range(OWNERS):
            rows = []
            for pair in range(bands // twin):
                cells = []
                for band in range(twin):
                    for part in range(2):
                        at = (part * bands + pair * twin + band) * slots
                        cells.append(placed[inner][at:at + slots])
                rows.append(jnp.concatenate(cells, 1))
            turned.append(dot(jnp.concatenate(rows, 0), depth_ref[...]).astype(BF16))
        for inner in range(OWNERS):
            where = pl.ds(pl.multiple_of((step * OWNERS + inner) * slots, slots), slots)
            for part in range(2):
                for pair in range(bands // twin):
                    loose[part, where, pl.ds(pair * NR, NR)] = turned[inner][
                        pair * slots:(pair + 1) * slots, part * NR:(part + 1) * NR
                    ]
        return carry

    lax.fori_loop(0, owners // OWNERS, spread, 0)
    permute(loose, packed_ref, rank_ref)


def plane_kernel(
    near_ref, close_ref, apart_ref, mine_ref, order_ref, xs_ref, ys_ref, packed, volume_ref,
    ahead_ref, behind_ref, first_ref, second_ref, depth_ref,
    out_ref,
    loose, picked, mixer, work, level, rows_one, rows_two, held,
):
    owners = mine_ref.shape[0]
    parts = mine_ref.shape[1] - 8
    sticks = order_ref.shape[1]
    slots = sticks // owners
    bands = parts // 2
    twin = depth_ref.shape[1] // (2 * NR)
    group = held.shape[0]

    def make_rows(step, carry):
        rows = pl.ds(pl.multiple_of(step * BLOCK, BLOCK), BLOCK)
        choice = hot(lax.broadcasted_iota(jnp.int32, (BLOCK, NR), 1) == xs_ref[rows, :])
        rows_one[rows, :] = dot(choice, first_ref[...]).astype(BF16)
        rows_two[rows, :] = dot(choice, second_ref[...]).astype(BF16)
        return carry

    lax.fori_loop(0, sticks // BLOCK, make_rows, 0)

    def make_mixer(step, carry):
        for inner in range(5):
            y = step * 5 + inner
            rows = pl.ds(pl.multiple_of(near_ref[y], 16), NR)
            mine = ys_ref[rows, :] == y
            mine = jnp.concatenate([mine, mine], 1)
            one = jnp.where(mine, rows_one[rows, :].astype(F32), 0.0)
            two = jnp.where(mine, rows_two[rows, :].astype(F32), 0.0)
            mixer[y] = jnp.concatenate([one.T, two.T], 1).astype(BF16)
        return carry

    lax.fori_loop(0, SIDE // 5, make_mixer, 0)

    def make_level(step, carry):
        for inner in range(8):
            rx = step * 8 + inner
            rows = [volume_ref[apart_ref[holder], rx].astype(F32) for holder in range(volume_ref.shape[0])]
            level[rx] = jnp.concatenate(rows * twin, 0).T
        return carry

    lax.fori_loop(0, NR // 8, make_level, 0)

    for half in range(2):
        for part in range(2):
            for row in range(SIDE, PAD):
                work[half, pl.ds(part * PAD + row + 2 * half, NR, stride=PITCH), :] = jnp.zeros((NR, NR), F32)

    def rows_of(step, inner, half):
        return pl.ds((step * group + inner) * PITCH + 2 * half, 2 * PAD)

    def lift(step):
        data = []
        for inner in range(group):
            data.append(
                jnp.concatenate([work[half, rows_of(step, inner, half), :] for half in range(2)], 1).astype(BF16)
            )
        for inner in range(group):
            psi = dot(ahead_ref[...], data[inner])
            here = level[step * group + inner]
            here = jnp.concatenate([here, here], 1)
            here = jnp.concatenate([here, here], 0)
            held[inner] = (psi * here).astype(BF16)

    def fall():
        return [dot(behind_ref[...], held[inner]) for inner in range(group)]

    def put(step, results):
        for inner in range(group):
            for half in range(2):
                work[half, rows_of(step, inner, half), :] = results[inner][:, half * NR:(half + 1) * NR]

    def tile(index, carry):
        lanes = pl.ds(pl.multiple_of(index * BLOCK, BLOCK), BLOCK)

        def stage_one(step, carry):
            results = []
            for inner in range(STEP):
                y = step * STEP + inner
                rows = pl.ds(pl.multiple_of(near_ref[y], 16), NR)
                data = jnp.concatenate([packed[0, rows, lanes], packed[1, rows, lanes]], 0)
                results.append(dot(mixer[y], data))
            for inner in range(STEP):
                y = step * STEP + inner
                for half in range(2):
                    for part in range(2):
                        work[half, pl.ds(part * PAD + y + 2 * half, NR, stride=PITCH), :] = results[inner][
                            part * NR:(part + 1) * NR, half * NR:(half + 1) * NR
                        ]
            return carry

        lax.fori_loop(0, SIDE // STEP, stage_one, 0)

        def stage_two(step, carry):
            results = fall()
            lift(step)
            put(step - 1, results)
            return carry

        lift(0)
        lax.fori_loop(1, NR // group, stage_two, 0)
        put(NR // group - 1, fall())

        def stage_three(step, carry):
            results = []
            for inner in range(STEP):
                y = step * STEP + inner
                data = [
                    jnp.concatenate(
                        [work[half, pl.ds(part * PAD + y + 2 * half, NR, stride=PITCH), :] for half in range(2)], 1
                    )
                    for part in range(2)
                ]
                data = jnp.concatenate(data, 0).astype(BF16)
                rows = pl.ds(pl.multiple_of(close_ref[y], 16), WIN)
                weights = jnp.concatenate([rows_one[rows, :], rows_two[rows, :]], 0)
                results.append(dot(weights, data))
            for inner in range(STEP):
                y = step * STEP + inner
                rows = pl.ds(pl.multiple_of(close_ref[y], 16), WIN)
                mine = ys_ref[rows, :] == y
                mine = jnp.concatenate([mine, mine], 1)
                for part in range(2):
                    pltpu.store(
                        picked.at[part, rows, lanes],
                        results[inner][part * WIN:(part + 1) * WIN],
                        mask=mine,
                    )
            return carry

        lax.fori_loop(0, SIDE // STEP, stage_three, 0)
        return carry

    lax.fori_loop(0, packed.shape[2] // BLOCK, tile, 0)

    permute(picked, loose, order_ref)

    def collect(step, carry):
        total = hot(
            lax.broadcasted_iota(jnp.int32, (parts, parts * slots), 1) // slots
            == lax.broadcasted_iota(jnp.int32, (parts, parts * slots), 0)
        )
        turned = []
        for inner in range(OWNERS):
            where = pl.ds(pl.multiple_of((step * OWNERS + inner) * slots, slots), slots)
            rows = []
            for pair in range(bands // twin):
                here = pl.ds(pair * NR, NR)
                rows.append(jnp.concatenate([loose[0, where, here], loose[1, where, here]], 1))
            turned.append(dot(jnp.concatenate(rows, 0), depth_ref[...]).astype(BF16))
        waved = []
        for inner in range(OWNERS):
            depth, slot = masks(mine_ref, step * OWNERS + inner, parts, slots)
            rows = []
            for part in range(2):
                for pair in range(bands // twin):
                    for band in range(twin):
                        at = (band * 2 + part) * NR
                        rows.append(turned[inner][pair * slots:(pair + 1) * slots, at:at + NR])
            found = dot(jnp.concatenate(rows, 0), depth)
            slot = jnp.concatenate([slot] * parts, 0)
            waved.append(jnp.where(slot, found, 0.0).astype(BF16))
        for inner in range(OWNERS):
            out_ref[step * OWNERS + inner] = dot(total, waved[inner]).astype(BF16)
        return carry

    lax.fori_loop(0, owners // OWNERS, collect, 0)


def return_kernel(made_ref, back_ref, arrived, total, twin_send, twin_recv, send_sem, recv_sem):
    columns = back_ref.shape[0]
    turn = lax.axis_index("tg")
    here = lax.axis_index("pw")

    swap = pltpu.make_async_remote_copy(
        src_ref=made_ref.at[pl.ds(columns, columns)],
        dst_ref=arrived,
        send_sem=twin_send,
        recv_sem=twin_recv,
        device_id=(1 - turn, here),
        device_id_type=pl.DeviceIdType.MESH,
    )
    swap.start()
    swap.wait()

    def add(at, carry):
        total[at] = (made_ref[at].astype(F32) + arrived[at].astype(F32)).astype(BF16)
        return carry

    lax.fori_loop(0, columns, add, 0)

    def copy(shift):
        peer = lax.rem(here + shift, columns)
        return pltpu.make_async_remote_copy(
            src_ref=total.at[peer],
            dst_ref=back_ref.at[here],
            send_sem=send_sem.at[shift],
            recv_sem=recv_sem.at[shift],
            device_id=(turn, peer),
            device_id_type=pl.DeviceIdType.MESH,
        )

    def push(shift, carry):
        copy(shift).start()
        return carry

    lax.fori_loop(1, columns, push, 0)
    back_ref[here] = total[here]

    def finish(shift, carry):
        copy(shift).wait_send()
        pltpu.make_async_remote_copy(
            src_ref=total.at[here],
            dst_ref=back_ref.at[lax.rem(here - shift + columns, columns)],
            send_sem=send_sem.at[shift],
            recv_sem=recv_sem.at[shift],
            device_id=(turn, here),
            device_id_type=pl.DeviceIdType.MESH,
        ).wait_recv()
        return carry

    lax.fori_loop(1, columns, finish, 0)


def body(coeffs, g_place, stick_column, potential):
    groups = lax.axis_size("tg")
    columns = lax.axis_size("pw")
    owners = groups * columns
    waves = g_place.shape[0]
    slots = stick_column.shape[0]
    bands = coeffs.shape[2] // columns
    sticks = owners * slots
    parts = 2 * bands

    minor = 1
    while minor * minor < columns:
        minor *= 2
    major = columns // minor

    def swap(value, axis, shift):
        size = lax.axis_size(axis)
        return lax.ppermute(value, axis, [(at, at ^ shift) for at in range(size)])

    local = potential.transpose(0, 2, 1).astype(BF16)[None]
    column = [local] + [swap(local, "pw", at * minor) for at in range(1, major)]
    column = jnp.concatenate(column)

    sent = coeffs.astype(BF16).transpose(2, 0, 1).reshape(columns, bands, 2, waves)
    sent = sent.transpose(0, 2, 1, 3).reshape(columns, parts, waves)
    marks = jnp.stack(
        [
            g_place // NR,
            g_place % NR,
            jnp.pad(stick_column // NR, (0, waves - slots)),
            jnp.pad(stick_column % NR, (0, waves - slots)),
        ]
    )
    marks = jnp.pad(marks, ((0, 4), (0, 0))).astype(BF16)
    marks = jnp.broadcast_to(marks[None], (columns, 8, waves))
    sent = jnp.concatenate([sent, marks], 1)
    others = [swap(column, "pw", at) for at in range(1, minor)]
    apart = jnp.bitwise_xor(jnp.arange(columns, dtype=jnp.int32), lax.axis_index("pw"))
    apart = apart % minor * major + apart // minor

    mine = lax.all_to_all(sent, "pw", split_axis=0, concat_axis=0, tiled=True)
    other = [swap(mine, "tg", at) for at in range(1, groups)]
    mine = jnp.concatenate([mine] + other)

    sites = mine[:, parts + 2:parts + 4, :slots].astype(F32).astype(jnp.int32)
    xs = jnp.bitwise_and(sites[:, 0].reshape(sticks) + HALF, NR - 1)
    ys = jnp.bitwise_and(sites[:, 1].reshape(sticks) + HALF, NR - 1)
    key = ys * NR + xs
    rank = jnp.sum((key[None, :] < key[:, None]).astype(jnp.int32), 1)
    spot = jnp.arange(sticks, dtype=jnp.int32)
    hit = rank[None, :] == spot[:, None]
    order = jnp.sum(jnp.where(hit, spot[None, :], 0), 1)
    sorted_key = jnp.sum(jnp.where(hit, key[None, :], 0), 1)
    wide = jnp.broadcast_to(sorted_key[:, None], (sticks, NR))
    starts = jnp.sum((ys[None, :] < jnp.arange(SIDE)[:, None]).astype(jnp.int32), 1) // 16 * 16
    near = jnp.minimum(starts, sticks - NR)
    close = jnp.minimum(starts, sticks - WIN)

    depth = depth_tables(groups)
    turn = lax.axis_index("tg")
    depth_ahead = jnp.asarray(depth, BF16)[turn]
    depth_behind = jnp.asarray(depth.transpose(0, 2, 1), BF16)[turn]

    smem = pl.BlockSpec(memory_space=pltpu.SMEM)
    vmem = pl.BlockSpec(memory_space=pltpu.VMEM)
    lanes = bands * (NR // groups)
    packed = pl.pallas_call(
        rise_kernel,
        out_shape=jax.ShapeDtypeStruct((2, sticks, lanes), BF16),
        in_specs=[vmem] * 3,
        out_specs=vmem,
        scratch_shapes=[pltpu.VMEM((2, sticks, lanes), BF16)],
        compiler_params=pltpu.CompilerParams(vmem_limit_bytes=48 * 2**20),
        cost_estimate=pl.CostEstimate(flops=2 * 10**10, bytes_accessed=4 * 2**20, transcendentals=0),
        name="rise",
    )(mine, rank[None, :], depth_ahead)
    packed, others = lax.optimization_barrier((packed, others))
    volume = jnp.concatenate([column] + others)

    made = pl.pallas_call(
        plane_kernel,
        out_shape=jax.ShapeDtypeStruct((owners, parts, waves), BF16),
        in_specs=[smem, smem, smem] + [vmem] * 11,
        out_specs=vmem,
        scratch_shapes=[
            pltpu.VMEM((2, sticks, lanes), BF16),
            pltpu.VMEM((2, sticks, lanes), F32),
            pltpu.VMEM((SIDE, 2 * NR, 2 * NR), BF16),
            pltpu.VMEM((2, NR * PITCH + 8, NR), F32),
            pltpu.VMEM((NR, NR, NR), F32),
            pltpu.VMEM((sticks, 2 * NR), BF16),
            pltpu.VMEM((sticks, 2 * NR), BF16),
            pltpu.VMEM((32 if sticks <= 1024 else 8, 2 * NR, 2 * NR), BF16),
        ],
        compiler_params=pltpu.CompilerParams(vmem_limit_bytes=60 * 2**20),
        cost_estimate=pl.CostEstimate(flops=8 * 10**10, bytes_accessed=8 * 2**20, transcendentals=0),
        name="planes",
    )(
        near, close, apart, mine, order[None, :],
        jnp.bitwise_and(wide, NR - 1), wide // NR, packed, volume, *plane_tables(), depth_behind,
    )

    assert groups == 2
    back = pl.pallas_call(
        return_kernel,
        out_shape=jax.ShapeDtypeStruct((columns, parts, waves), BF16),
        in_specs=[vmem],
        out_specs=vmem,
        scratch_shapes=[
            pltpu.VMEM((columns, parts, waves), BF16),
            pltpu.VMEM((columns, parts, waves), BF16),
            pltpu.SemaphoreType.DMA,
            pltpu.SemaphoreType.DMA,
            pltpu.SemaphoreType.DMA((columns,)),
            pltpu.SemaphoreType.DMA((columns,)),
        ],
        compiler_params=pltpu.CompilerParams(vmem_limit_bytes=16 * 2**20, has_side_effects=True),
        name="give_back",
    )(made)
    back = back.reshape(columns, 2, bands, waves).transpose(1, 3, 0, 2)
    return back.reshape(2, waves, columns * bands).astype(F32) * (1.0 / NR**3)


def solution(mesh):
    placed = (P(None, AXES, None), P(AXES), P(AXES), P(None, None, AXES))
    return jax.shard_map(
        body, mesh=mesh, in_specs=placed, out_specs=P(None, AXES, None), check_vma=False
    )
```
